128 devices in a mesh: row: 8 (over y, x_hi), col: 16 (over z, x_lo, core).
Axes of the slice: x: 4 (x_hi: 2, x_lo: 2; x = x_hi * 2 + x_lo), y: 4, z: 4, core: 2. Of those that a mesh axis runs over, the one named last changes fastest.
Arguments:
- model_gradient: float32 [3, 512, 512, 256], P(None, 'row', 'col'), may hold values from -6 to 6
- filter_x: float32 [512, 512], replicated, may hold values from 0 to 1, as said below
- filter_y: float32 [512, 512], replicated, may hold values from 0 to 1, as said below
- filter_z: float32 [256, 256], replicated, may hold values from 0 to 1, as said below
- depth_scale: float32 [3, 256], replicated, may hold values from 0.3 to 3
Outputs:
- smoothed: float32 [3, 512, 512, 256], P(None, 'row', 'col')
The draws below stay inside these ranges and needn't reach their ends.
Inputs may be any that keep to these rules, and one draw needn't show every extreme that they name: `filter_x`: each row is a nonnegative smoothing kernel of its own width plus one half on the diagonal; rows sum to one. `filter_y`: each row is a nonnegative smoothing kernel of its own width plus one half on the diagonal; rows sum to one. `filter_z`: each row is a nonnegative smoothing kernel of its own width plus one half on the diagonal; rows sum to one.
All inputs are finite; a program needn't handle non-finite values.
Results may differ from the reference program's by a relative error of at most 0.0001.
Values sent between devices are 32-bit elements; how exact they have to be, the bound alone decides.
A program may use at most 128 MiB of HBM per device.

```python
import math
import jax
import jax.numpy as jnp
from jax import lax

PARAMS = 3
NX = 512
NY = 512
NZ = 256


def smoothing_matrix(key, length):
    key_width = jax.random.fold_in(key, 11)
    key_rough = jax.random.fold_in(key, 12)
    lower, upper = (0.5, 1.5)
    widths = length * jnp.exp(jax.random.uniform(key_width, (length, 1), jnp.float32, jnp.log(1.0 / 16.0), jnp.log(1.0 / 4.0)))
    places = jnp.arange(length, dtype=jnp.float32)
    apart = places[:, None] - places[None, :]
    rough = jax.random.uniform(key_rough, (length, length), jnp.float32, lower, upper)
    kernel = jnp.exp(-apart * apart / (2.0 * widths * widths)) * rough
    kernel = 0.5 * kernel / jnp.sum(kernel, axis=1, keepdims=True)
    return kernel + 0.5 * jnp.eye(length, dtype=jnp.float32)


def draw_filter_x(key, part):
    return smoothing_matrix(jax.random.fold_in(key, 1), NX)


def draw_filter_y(key, part):
    return smoothing_matrix(jax.random.fold_in(key, 2), NY)


def draw_filter_z(key, part):
    return smoothing_matrix(jax.random.fold_in(key, 3), NZ)


def steps_of(rng, dims, pieces, smallest, high):
    factor_of = 1.0
    for position, blocks in pieces:
        heights = jax.random.uniform(jax.random.fold_in(jax.random.fold_in(rng, 6), position), (blocks,), jnp.float32, smallest / len(pieces), high / len(pieces))
        factor_of = factor_of * jnp.repeat(jnp.exp(heights), dims[position] // blocks).reshape((-1,) + (1,) * (len(dims) - 1 - position))
    return factor_of


def normal_values(key, dims, deviation, limit, cuts=(), held_as=jnp.bfloat16):
    gain = steps_of(key, dims, cuts, -0.22, 0.18) if cuts else 1.0
    result = jax.random.normal(key, dims, jnp.float32) * deviation * gain
    return jnp.minimum(jnp.maximum(result, -limit), limit).astype(held_as)


def setup_inputs(seed: int = 0) -> dict:
    keys = jax.random.split(jax.random.key(seed), 6)
    return {
        "model_gradient": normal_values(keys[0], (PARAMS, NX, NY, NZ), 1.0, 6.0, ((1, 8), (2, 16)), jnp.float32),
        "filter_x": draw_filter_x(jax.random.fold_in(keys[5], 71), 0),
        "filter_y": draw_filter_y(jax.random.fold_in(keys[5], 71), 0),
        "filter_z": draw_filter_z(jax.random.fold_in(keys[5], 71), 0),
        "depth_scale": jnp.clip(jnp.exp(jax.random.uniform(keys[4], (PARAMS, NZ), jnp.float32, math.log(0.3), math.log(3.0))), 0.3, 3.0),
    }


def reference(model_gradient, filter_x, filter_y, filter_z, depth_scale):
    highest_accuracy = lax.Precision.HIGHEST
    results = []
    for index in range(PARAMS):
        field = model_gradient[index]
        depth_pass = jnp.einsum("abz,kz->abk", field, filter_z, precision=highest_accuracy)
        depth_pass = depth_pass * depth_scale[index][None, None, :]
        initial_sweep = jnp.einsum("ia,abk->ibk", filter_x, depth_pass, precision=highest_accuracy)
        second_pass = jnp.einsum("jb,ibk->ijk", filter_y, initial_sweep, precision=highest_accuracy)
        results.append(second_pass)
    return jnp.stack(results)
```

```python
import jax
import jax.numpy as jnp
from jax import lax
from jax.experimental import pallas as pl
from jax.experimental.pallas import tpu as pltpu
from jax.sharding import PartitionSpec as P

MESH = pl.DeviceIdType.MESH
F32, BF16 = jnp.float32, jnp.bfloat16
ORDER = ("xyz", "yzx", "zxy")
CHUNKS = [(half, p) for half in range(2) for p in range(3)]


def split(value):
    high = value.astype(BF16)
    return high, (value - high.astype(F32)).astype(BF16)


def swap_blocks(parts):
    lane = lax.broadcasted_iota(jnp.int32, parts[0].shape, 1)
    low64, low32 = lane < 64, lane % 64 < 32
    mid = [None] * 4
    for e in range(2):
        one, two = parts[e], parts[e + 2]
        mid[e] = jnp.where(low64, one, pltpu.roll(two, 64, 1))
        mid[e + 2] = jnp.where(low64, pltpu.roll(one, 64, 1), two)
    out = [None] * 4
    for e in (0, 2):
        one, two = mid[e], mid[e + 1]
        out[e] = jnp.where(low32, one, pltpu.roll(two, 32, 1))
        out[e + 1] = jnp.where(low32, pltpu.roll(one, 96, 1), two)
    return out


def dot3(a_high, a_low, b_high, b_low):
    def dot(a, b):
        return jnp.dot(a, b, preferred_element_type=F32)

    return dot(a_high, b_high) + dot(a_low, b_high) + dot(a_high, b_low)


def kernel(
    g_hbm, fx_hbm, fy_hbm, fz_hbm, scale_ref, out_hbm,
    s0, r1, r2, r3, b1, b2, b3,
    wbuf, fxh, fxl, fyh, fyl, fzh, fzl, ph, pll, qh, ql, obuf,
    send_sem, recv_sem, in_sem, w_sem, out_sem,
):
    row, col = lax.axis_index("row"), lax.axis_index("col")
    me = {"x": (row % 2) * 2 + (col // 2) % 2, "y": row // 2, "z": col // 4}
    core = col % 2

    def device(at, k):
        x = at["x"]
        return (at["y"] * 2 + x // 2, at["z"] * 4 + (x % 2) * 2 + k)

    def along(dim, step, flip):
        at = dict(me)
        at[dim] = (me[dim] + step) % 4
        return at, (core + flip) % 2

    barrier = pltpu.get_barrier_semaphore()
    partners = [along(d, s, f) for d in "xyz" for s in (1, 2, 3) for f in (0, 1)]
    partners.append(along("x", 0, 1))
    for at, k in partners:
        pl.semaphore_signal(barrier, inc=1, device_id=device(at, k), device_id_type=MESH)

    def load_in(p, j):
        c = j * 3 + p
        return pltpu.make_async_copy(
            g_hbm.at[p, :, pl.ds(j * 128, 128)], b3.at[c], in_sem.at[c]
        )

    fz_copy = pltpu.make_async_copy(fz_hbm, wbuf.at[2, pl.ds(0, 256), pl.ds(0, 256)], w_sem.at[2])
    fz_copy.start()
    for p in range(3):
        for j in range(2):
            load_in(p, j).start()
    fx_copy = pltpu.make_async_copy(fx_hbm, wbuf.at[0], w_sem.at[0])
    fy_copy = pltpu.make_async_copy(fy_hbm, wbuf.at[1], w_sem.at[1])
    fx_copy.start()
    fy_copy.start()

    def transfers(c, stage):
        order = ORDER[c % 3]
        dim = order[(0, 1, 2, 2, 1, 0)[stage]]
        mine = me[dim]
        found = []
        for step in (1, 3, 2, 0):
            for flip in (0, 1) if stage in (0, 5) else (0,):
                if step == 0 and flip == 0:
                    continue
                at, k = along(dim, step, flip)
                d = at[dim]
                slot, own = d * 2 + k, mine * 2 + core
                if stage == 0:
                    src, dst = s0.at[c, pl.ds(slot * 256, 256)], r1.at[c, own]
                elif stage == 1:
                    src, dst = r1.at[c, :, pl.ds(d * 64, 64)], r2.at[c, :, mine]
                elif stage == 2:
                    src, dst = r2.at[c, :, :, pl.ds(d * 16, 16)], r3.at[c, :, :, mine]
                elif stage == 3:
                    src, dst = r3.at[c, :, :, d], b1.at[c, :, :, pl.ds(mine * 16, 16)]
                elif stage == 4:
                    src, dst = b1.at[c, :, d], b2.at[c, :, pl.ds(mine * 64, 64)]
                else:
                    src, dst = b2.at[c, slot], b3.at[c, pl.ds(own * 256, 256)]
                found.append(
                    pltpu.make_async_remote_copy(
                        src, dst, send_sem.at[c, stage], recv_sem.at[c, stage],
                        device_id=device(at, k), device_id_type=MESH,
                    )
                )
        return found

    def send(c, stage):
        for copy in transfers(c, stage):
            copy.start()
        keep(c, stage)

    def keep(c, stage):
        mine = me[ORDER[c % 3][(0, 1, 2, 2, 1, 0)[stage]]]
        own = mine * 2 + core
        if stage == 0:
            r1[c, own] = s0[c, pl.ds(pl.multiple_of(own * 256, 256), 256)]
        elif stage == 5:
            b3[c, pl.ds(pl.multiple_of(own * 256, 256), 256)] = b2[c, own]
        else:

            @pl.loop(0, 8)
            def _(i):
                if stage == 1:
                    r2[c, i, mine] = r1[c, i, pl.ds(pl.multiple_of(mine * 64, 64), 64)]
                elif stage == 2:
                    for k in range(4):
                        r3[c, i, k, mine] = r2[c, i, k, pl.ds(pl.multiple_of(mine * 16, 16), 16)]
                elif stage == 3:
                    for k in range(4):
                        b1[c, i, k, pl.ds(pl.multiple_of(mine * 16, 16), 16)] = r3[c, i, k, mine]
                else:
                    b2[c, i, pl.ds(pl.multiple_of(mine * 64, 64), 64)] = b1[c, i, mine]

    def arrived(c, stage):
        ref = (
            r1.at[c, pl.ds(0, 7)], r2.at[c, pl.ds(0, 6)], r3.at[c, pl.ds(0, 6)],
            b1.at[c, pl.ds(0, 6)], b2.at[c, pl.ds(0, 6)], b3.at[c, pl.ds(0, 7 * 256)],
        )[stage]
        pltpu.make_async_copy(ref, ref, recv_sem.at[c, stage]).wait()

    def sent(c, stage):
        ref = (
            r1.at[c, pl.ds(0, 7)], r2.at[c, pl.ds(0, 6)], r3.at[c, pl.ds(0, 6)],
            b1.at[c, pl.ds(0, 6)], b2.at[c, pl.ds(0, 6)], b3.at[c, pl.ds(0, 7 * 256)],
        )[stage]
        pltpu.make_async_copy(ref, ref, send_sem.at[c, stage]).wait()

    fz_copy.wait()
    fzh[...], fzl[...] = split(wbuf[2, 0:256, 0:256])

    def depth(p):
        for j in range(2):
            load_in(p, j).wait()

        @pl.loop(0, 8)
        def _(it):
            rows = []
            for u in range(2):
                for b in range(4):
                    at = pl.multiple_of((b * 16 + it * 2 + u) * 32, 32)
                    rows.append(
                        jnp.concatenate([b3[p, pl.ds(at, 32)], b3[3 + p, pl.ds(at, 32)]], axis=1)
                    )
            high, low = split(jnp.concatenate(rows, axis=0))

            def dot(a, b):
                return lax.dot_general(
                    a, b, (((1,), (1,)), ((), ())), preferred_element_type=F32
                )

            for j in range(2):
                fh, fl = fzh[pl.ds(j * 128, 128)], fzl[pl.ds(j * 128, 128)]
                got = dot(fh, high) + dot(fl, high) + dot(fh, low)
                for u in range(2):
                    s0[j * 3 + p, pl.ds(it * 2 + u, 128, stride=16)] = got[:, u * 128 : u * 128 + 128]

    depth(0)
    pl.semaphore_wait(barrier, len(partners))
    send(0, 0)
    depth(1)
    send(1, 0)
    depth(2)
    send(2, 0)
    for c in (3, 4, 5):
        send(c, 0)

    fx_copy.wait()
    fy_copy.wait()

    @pl.loop(0, 4)
    def _(i):
        at = pl.ds(pl.multiple_of(i * 128, 128), 128)
        fxh[at], fxl[at] = split(wbuf[0, at])
        turned = jnp.concatenate([wbuf[1, pl.ds(k * 128, 128), at].T for k in range(4)], axis=1)
        fyh[at], fyl[at] = split(turned)

    def units(c, r, q):
        found = []
        for e in range(4):
            at = {"x": (r % 2) * 2 + e // 2, "y": r // 2, "z": q}
            one, two, three = (at[d] for d in ORDER[c % 3])
            found.append((one * 2 + e % 2, two, three))
        return found

    def smooth(c):
        @pl.loop(0, 8)
        def _(r):
            for q in range(4):
                blocks = swap_blocks([r3[c, i, k, m] for i, k, m in units(c, r, q)])
                for b in range(4):
                    at = pl.ds(pl.multiple_of(r * 64 + b * 16, 16), 16)
                    high, low = split(blocks[b])
                    ph[at, q * 128 : q * 128 + 128] = high
                    pll[at, q * 128 : q * 128 + 128] = low

        @pl.loop(0, 2)
        def _(ib):
            at = pl.ds(pl.multiple_of(ib * 256, 256), 256)
            for n in range(2):
                cut = slice(n * 256, n * 256 + 256)
                qh[:, cut], ql[:, cut] = split(dot3(fxh[at], fxl[at], ph[:, cut], pll[:, cut]))
            for n in range(2):
                cut = slice(n * 256, n * 256 + 256)
                obuf[:, cut] = dot3(qh[...], ql[...], fyh[:, cut], fyl[:, cut])

            @pl.loop(0, 4)
            def _(rr):
                r = ib * 4 + rr
                for q in range(4):
                    blocks = swap_blocks(
                        [
                            obuf[pl.ds(pl.multiple_of(rr * 64 + b * 16, 16), 16), q * 128 : q * 128 + 128]
                            for b in range(4)
                        ]
                    )
                    for e, (i, k, m) in enumerate(units(c, r, q)):
                        r3[c, i, k, m] = blocks[e]

    for stage in (1, 2):
        for c in range(6):
            arrived(c, stage - 1)
            send(c, stage)
    for c in range(6):
        arrived(c, 2)
        smooth(c)
        send(c, 3)
    for stage in (4, 5):
        for c in range(6):
            arrived(c, stage - 1)
            send(c, stage)

    def store_out(c):
        half, p = CHUNKS[c]
        return pltpu.make_async_copy(
            r1.at[c], out_hbm.at[p, :, :, pl.ds(half * 128, 128)], out_sem.at[c]
        )

    for c in range(6):
        half, p = CHUNKS[c]
        sent(c, 1)
        arrived(c, 5)

        @pl.loop(0, 16)
        def _(m):
            turned = b3[c, pl.ds(m, 128, stride=16)].T
            turned = turned * scale_ref[p : p + 1, half * 128 : half * 128 + 128]
            for b in range(4):
                at = pl.multiple_of((m % 8) * 32, 32)
                r1[c, b * 2 + m // 8, pl.ds(at, 32)] = turned[b * 32 : b * 32 + 32]

        store_out(c).start()
    for c in range(6):
        for stage in (0, 2, 3, 4, 5):
            sent(c, stage)
        store_out(c).wait()


def shards(model_gradient, filter_x, filter_y, filter_z, depth_scale):
    params, xloc, yloc, depth = model_gradient.shape
    anywhere = pl.BlockSpec(memory_space=pl.ANY)
    result = pl.pallas_call(
        kernel,
        out_shape=jax.ShapeDtypeStruct((params, 8, 256, depth), F32),
        in_specs=[anywhere] * 4 + [pl.BlockSpec(memory_space=pltpu.VMEM)],
        out_specs=anywhere,
        scratch_shapes=[
            pltpu.VMEM((6, 2048, 128), F32),
            pltpu.VMEM((6, 8, 256, 128), F32),
            pltpu.VMEM((6, 8, 4, 64, 128), F32),
            pltpu.VMEM((6, 8, 4, 4, 16, 128), F32),
            pltpu.VMEM((6, 8, 4, 64, 128), F32),
            pltpu.VMEM((6, 8, 256, 128), F32),
            pltpu.VMEM((6, 2048, 128), F32),
            pltpu.VMEM((3, 512, 512), F32),
            pltpu.VMEM((512, 512), BF16),
            pltpu.VMEM((512, 512), BF16),
            pltpu.VMEM((512, 512), BF16),
            pltpu.VMEM((512, 512), BF16),
            pltpu.VMEM((256, 256), BF16),
            pltpu.VMEM((256, 256), BF16),
            pltpu.VMEM((512, 512), BF16),
            pltpu.VMEM((512, 512), BF16),
            pltpu.VMEM((256, 512), BF16),
            pltpu.VMEM((256, 512), BF16),
            pltpu.VMEM((256, 512), F32),
            pltpu.SemaphoreType.DMA((6, 6)),
            pltpu.SemaphoreType.DMA((6, 6)),
            pltpu.SemaphoreType.DMA((6,)),
            pltpu.SemaphoreType.DMA((3,)),
            pltpu.SemaphoreType.DMA((6,)),
        ],
        compiler_params=pltpu.CompilerParams(
            collective_id=0, has_side_effects=True, vmem_limit_bytes=60 * 2**20
        ),
        name="smooth_planes",
    )(model_gradient.reshape(params, xloc * yloc, depth), filter_x, filter_y, filter_z, depth_scale)
    return result.reshape(params, xloc, yloc, depth)


def solution(mesh):
    return jax.shard_map(
        shards,
        mesh=mesh,
        in_specs=(P(None, "row", "col", None), P(), P(), P(), P()),
        out_specs=P(None, "row", "col", None),
        check_vma=False,
    )
```

```python
import jax
import jax.numpy as jnp
from jax import lax
from jax.experimental import pallas as pl
from jax.experimental.pallas import tpu as pltpu
from jax.sharding import PartitionSpec as P

MESH = pl.DeviceIdType.MESH
F32, BF16 = jnp.float32, jnp.bfloat16
ORDER = ("xyz", "yzx", "zxy")
CHUNKS = [(half, p) for half in range(2) for p in range(3)]


def split(value):
    high = value.astype(BF16)
    return high, (value - high.astype(F32)).astype(BF16)


def swap_blocks(parts):
    lane = lax.broadcasted_iota(jnp.int32, parts[0].shape, 1)
    low64, low32 = lane < 64, lane % 64 < 32
    mid = [None] * 4
    for e in range(2):
        one, two = parts[e], parts[e + 2]
        mid[e] = jnp.where(low64, one, pltpu.roll(two, 64, 1))
        mid[e + 2] = jnp.where(low64, pltpu.roll(one, 64, 1), two)
    out = [None] * 4
    for e in (0, 2):
        one, two = mid[e], mid[e + 1]
        out[e] = jnp.where(low32, one, pltpu.roll(two, 32, 1))
        out[e + 1] = jnp.where(low32, pltpu.roll(one, 96, 1), two)
    return out


def dot3(a_high, a_low, b_high, b_low):
    def dot(a, b):
        return jnp.dot(a, b, preferred_element_type=F32)

    return dot(a_high, b_high) + dot(a_low, b_high) + dot(a_high, b_low)


def kernel(
    g_hbm, fx_hbm, fy_hbm, fz_hbm, scale_ref, out,
    s0, r1, r2, r3, b1, b2, b3,
    wbuf, fxh, fxl, fyh, fyl, fzh, fzl, ph, pll, qh, ql, obuf,
    send_sem, recv_sem, in_sem, w_sem,
):
    row, col = lax.axis_index("row"), lax.axis_index("col")
    me = {"x": (row % 2) * 2 + (col // 2) % 2, "y": row // 2, "z": col // 4}
    core = col % 2

    def device(at, k):
        x = at["x"]
        return (at["y"] * 2 + x // 2, at["z"] * 4 + (x % 2) * 2 + k)

    def along(dim, step, flip):
        at = dict(me)
        at[dim] = (me[dim] + step) % 4
        return at, (core + flip) % 2

    barrier = pltpu.get_barrier_semaphore()
    partners = [along(d, s, f) for d in "xyz" for s in (1, 2, 3) for f in (0, 1)]
    partners.append(along("x", 0, 1))
    for at, k in partners:
        pl.semaphore_signal(barrier, inc=1, device_id=device(at, k), device_id_type=MESH)

    def load_in(p, j):
        c = j * 3 + p
        return pltpu.make_async_copy(
            g_hbm.at[p, :, pl.ds(j * 128, 128)], b3.at[c], in_sem.at[c]
        )

    fz_copy = pltpu.make_async_copy(fz_hbm, wbuf.at[2, pl.ds(0, 256), pl.ds(0, 256)], w_sem.at[2])
    fz_copy.start()
    for p in range(3):
        for j in range(2):
            load_in(p, j).start()
    fx_copy = pltpu.make_async_copy(fx_hbm, wbuf.at[0], w_sem.at[0])
    fy_copy = pltpu.make_async_copy(fy_hbm, wbuf.at[1], w_sem.at[1])
    fx_copy.start()
    fy_copy.start()

    def transfers(c, stage):
        order = ORDER[c % 3]
        dim = order[(0, 1, 2, 2, 1, 0)[stage]]
        mine = me[dim]
        found = []
        for step in (1, 3, 2, 0):
            for flip in (0, 1) if stage in (0, 5) else (0,):
                if step == 0 and flip == 0:
                    continue
                at, k = along(dim, step, flip)
                d = at[dim]
                slot, own = d * 2 + k, mine * 2 + core
                if stage == 0:
                    src, dst = s0.at[c, pl.ds(slot * 256, 256)], r1.at[c, own]
                elif stage == 1:
                    src, dst = r1.at[c, :, pl.ds(d * 64, 64)], r2.at[c, :, mine]
                elif stage == 2:
                    src, dst = r2.at[c, :, :, pl.ds(d * 16, 16)], r3.at[c, :, :, mine]
                elif stage == 3:
                    src, dst = r3.at[c, :, :, d], b1.at[c, :, :, pl.ds(mine * 16, 16)]
                elif stage == 4:
                    src, dst = b1.at[c, :, d], b2.at[c, :, pl.ds(mine * 64, 64)]
                else:
                    src, dst = b2.at[c, slot], b3.at[c, pl.ds(own * 256, 256)]
                found.append(
                    pltpu.make_async_remote_copy(
                        src, dst, send_sem.at[c, stage], recv_sem.at[c, stage],
                        device_id=device(at, k), device_id_type=MESH,
                    )
                )
        return found

    def send(c, stage):
        with jax.named_scope(f"send#c={c}#s={stage}"):
            for copy in transfers(c, stage):
                copy.start()
        with jax.named_scope(f"keep#c={c}#s={stage}"):
            keep(c, stage)

    def keep(c, stage):
        mine = me[ORDER[c % 3][(0, 1, 2, 2, 1, 0)[stage]]]
        own = mine * 2 + core
        if stage == 0:
            r1[c, own] = s0[c, pl.ds(pl.multiple_of(own * 256, 256), 256)]
        elif stage == 5:
            b3[c, pl.ds(pl.multiple_of(own * 256, 256), 256)] = b2[c, own]
        else:

            @pl.loop(0, 8)
            def _(i):
                if stage == 1:
                    r2[c, i, mine] = r1[c, i, pl.ds(pl.multiple_of(mine * 64, 64), 64)]
                elif stage == 2:
                    for k in range(4):
                        r3[c, i, k, mine] = r2[c, i, k, pl.ds(pl.multiple_of(mine * 16, 16), 16)]
                elif stage == 3:
                    for k in range(4):
                        b1[c, i, k, pl.ds(pl.multiple_of(mine * 16, 16), 16)] = r3[c, i, k, mine]
                else:
                    b2[c, i, pl.ds(pl.multiple_of(mine * 64, 64), 64)] = b1[c, i, mine]

    def arrived(c, stage):
        ref = (
            r1.at[c, pl.ds(0, 7)], r2.at[c, pl.ds(0, 6)], r3.at[c, pl.ds(0, 6)],
            b1.at[c, pl.ds(0, 6)], b2.at[c, pl.ds(0, 6)], b3.at[c, pl.ds(0, 7 * 256)],
        )[stage]
        with jax.named_scope(f"arrive#c={c}#s={stage}"):
            pltpu.make_async_copy(ref, ref, recv_sem.at[c, stage]).wait()

    def sent(c, stage):
        ref = (
            r1.at[c, pl.ds(0, 7)], r2.at[c, pl.ds(0, 6)], r3.at[c, pl.ds(0, 6)],
            b1.at[c, pl.ds(0, 6)], b2.at[c, pl.ds(0, 6)], b3.at[c, pl.ds(0, 7 * 256)],
        )[stage]
        pltpu.make_async_copy(ref, ref, send_sem.at[c, stage]).wait()

    fz_copy.wait()
    fzh[...], fzl[...] = split(wbuf[2, 0:256, 0:256])

    def depth(p, j):
        fh, fl = fzh[j * 128 : j * 128 + 128], fzl[j * 128 : j * 128 + 128]

        @pl.loop(0, 8, unroll=4)
        def _(it):
            rows = []
            for u in range(2):
                for b in range(4):
                    at = pl.multiple_of((b * 16 + it * 2 + u) * 32, 32)
                    rows.append(
                        jnp.concatenate([b3[p, pl.ds(at, 32)], b3[3 + p, pl.ds(at, 32)]], axis=1)
                    )
            high, low = split(jnp.concatenate(rows, axis=0))

            def dot(a, b):
                return lax.dot_general(
                    a, b, (((1,), (1,)), ((), ())), preferred_element_type=F32
                )

            got = dot(fh, high) + dot(fl, high) + dot(fh, low)
            for u in range(2):
                s0[j * 3 + p, pl.ds(it * 2 + u, 128, stride=16)] = got[:, u * 128 : u * 128 + 128]

    for c in range(6):
        half, p = CHUNKS[c]
        if half == 0:
            for j in range(2):
                load_in(p, j).wait()
        with jax.named_scope(f"depth#c={c}"):
            depth(p, half)
        if c == 0:
            pl.semaphore_wait(barrier, len(partners))
        send(c, 0)

    with jax.named_scope("weights"):
        fx_copy.wait()
        fy_copy.wait()

        @pl.loop(0, 4)
        def _(i):
            at = pl.ds(pl.multiple_of(i * 128, 128), 128)
            fxh[at], fxl[at] = split(wbuf[0, at])
            turned = jnp.concatenate([wbuf[1, pl.ds(k * 128, 128), at].T for k in range(4)], axis=1)
            fyh[at], fyl[at] = split(turned)

    def units(c, r, q):
        found = []
        for e in range(4):
            at = {"x": (r % 2) * 2 + e // 2, "y": r // 2, "z": q}
            one, two, three = (at[d] for d in ORDER[c % 3])
            found.append((one * 2 + e % 2, two, three))
        return found

    def smooth(c):
        @pl.loop(0, 8, unroll=2)
        def _(r):
            for q in range(4):
                blocks = swap_blocks([r3[c, i, k, m] for i, k, m in units(c, r, q)])
                for b in range(4):
                    at = pl.ds(pl.multiple_of(r * 64 + b * 16, 16), 16)
                    high, low = split(blocks[b])
                    ph[at, q * 128 : q * 128 + 128] = high
                    pll[at, q * 128 : q * 128 + 128] = low

        @pl.loop(0, 2)
        def _(ib):
            at = pl.ds(pl.multiple_of(ib * 256, 256), 256)
            for n in range(2):
                cut = slice(n * 256, n * 256 + 256)
                qh[:, cut], ql[:, cut] = split(dot3(fxh[at], fxl[at], ph[:, cut], pll[:, cut]))
            for n in range(2):
                cut = slice(n * 256, n * 256 + 256)
                obuf[:, cut] = dot3(qh[...], ql[...], fyh[:, cut], fyl[:, cut])

            @pl.loop(0, 4, unroll=2)
            def _(rr):
                r = ib * 4 + rr
                for q in range(4):
                    blocks = swap_blocks(
                        [
                            obuf[pl.ds(pl.multiple_of(rr * 64 + b * 16, 16), 16), q * 128 : q * 128 + 128]
                            for b in range(4)
                        ]
                    )
                    for e, (i, k, m) in enumerate(units(c, r, q)):
                        r3[c, i, k, m] = blocks[e]

    for stage in (1, 2):
        for c in range(6):
            arrived(c, stage - 1)
            send(c, stage)
    for c in range(6):
        arrived(c, 2)
        with jax.named_scope(f"smooth#c={c}"):
            smooth(c)
        send(c, 3)
    for stage in (4, 5):
        for c in range(6):
            arrived(c, stage - 1)
            send(c, stage)

    for c in range(6):
        half, p = CHUNKS[c]
        arrived(c, 5)

        with jax.named_scope(f"final#c={c}"):

            @pl.loop(0, 16, unroll=4)
            def _(m):
                turned = b3[c, pl.ds(m, 128, stride=16)].T
                turned = turned * scale_ref[p : p + 1, half * 128 : half * 128 + 128]
                for b in range(4):
                    at = pl.multiple_of((m % 8) * 32, 32)
                    out[p, b * 2 + m // 8, pl.ds(at, 32), half * 128 : half * 128 + 128] = turned[
                        b * 32 : b * 32 + 32
                    ]
    with jax.named_scope("drain"):
        for c in range(6):
            for stage in range(6):
                sent(c, stage)


def shards(model_gradient, filter_x, filter_y, filter_z, depth_scale):
    params, xloc, yloc, depth = model_gradient.shape
    anywhere = pl.BlockSpec(memory_space=pl.ANY)
    result = pl.pallas_call(
        kernel,
        out_shape=pltpu.VMEM((params, 8, 256, depth), F32),
        in_specs=[anywhere] * 4 + [pl.BlockSpec(memory_space=pltpu.VMEM)],
        out_specs=pl.BlockSpec(memory_space=pltpu.VMEM),
        scratch_shapes=[
            pltpu.VMEM((6, 2048, 128), F32),
            pltpu.VMEM((6, 8, 256, 128), F32),
            pltpu.VMEM((6, 8, 4, 64, 128), F32),
            pltpu.VMEM((6, 8, 4, 4, 16, 128), F32),
            pltpu.VMEM((6, 8, 4, 64, 128), F32),
            pltpu.VMEM((6, 8, 256, 128), F32),
            pltpu.VMEM((6, 2048, 128), F32),
            pltpu.VMEM((3, 512, 512), F32),
            pltpu.VMEM((512, 512), BF16),
            pltpu.VMEM((512, 512), BF16),
            pltpu.VMEM((512, 512), BF16),
            pltpu.VMEM((512, 512), BF16),
            pltpu.VMEM((256, 256), BF16),
            pltpu.VMEM((256, 256), BF16),
            pltpu.VMEM((512, 512), BF16),
            pltpu.VMEM((512, 512), BF16),
            pltpu.VMEM((256, 512), BF16),
            pltpu.VMEM((256, 512), BF16),
            pltpu.VMEM((256, 512), F32),
            pltpu.SemaphoreType.DMA((6, 6)),
            pltpu.SemaphoreType.DMA((6, 6)),
            pltpu.SemaphoreType.DMA((6,)),
            pltpu.SemaphoreType.DMA((3,)),
        ],
        compiler_params=pltpu.CompilerParams(
            collective_id=0, has_side_effects=True, vmem_limit_bytes=53 * 2**20
        ),
        name="smooth_planes",
    )(model_gradient.reshape(params, xloc * yloc, depth), filter_x, filter_y, filter_z, depth_scale)
    return result.reshape(params, xloc, yloc, depth)


def solution(mesh):
    return jax.shard_map(
        shards,
        mesh=mesh,
        in_specs=(P(None, "row", "col", None), P(), P(), P(), P()),
        out_specs=P(None, "row", "col", None),
        check_vma=False,
    )
```

```python
import jax
import jax.numpy as jnp
from jax import lax
from jax.experimental import pallas as pl
from jax.experimental.pallas import tpu as pltpu
from jax.sharding import PartitionSpec as P

MESH = pl.DeviceIdType.MESH
F32, BF16 = jnp.float32, jnp.bfloat16
ORDER = ("xyz", "yzx", "zxy")
CHUNKS = [(half, p) for half in range(2) for p in range(3)]


def split(value):
    high = value.astype(BF16)
    return high, (value - high.astype(F32)).astype(BF16)


def swap_blocks(parts):
    lane = lax.broadcasted_iota(jnp.int32, parts[0].shape, 1)
    low64, low32 = lane < 64, lane % 64 < 32
    mid = [None] * 4
    for e in range(2):
        one, two = parts[e], parts[e + 2]
        mid[e] = jnp.where(low64, one, pltpu.roll(two, 64, 1))
        mid[e + 2] = jnp.where(low64, pltpu.roll(one, 64, 1), two)
    out = [None] * 4
    for e in (0, 2):
        one, two = mid[e], mid[e + 1]
        out[e] = jnp.where(low32, one, pltpu.roll(two, 32, 1))
        out[e + 1] = jnp.where(low32, pltpu.roll(one, 96, 1), two)
    return out


def dot3(a_high, a_low, b_high, b_low):
    def dot(a, b):
        return jnp.dot(a, b, preferred_element_type=F32)

    return dot(a_high, b_high) + dot(a_low, b_high) + dot(a_high, b_low)


def kernel(
    g_hbm, fx_hbm, fy_hbm, fz_hbm, scale_ref, out,
    s0, r1, r2, r3, b1, b2, b3,
    wbuf, fxh, fxl, fyh, fyl, fzh, fzl, ph, pll, qh, ql, pbuf,
    send_sem, recv_sem, in_sem, w_sem,
):
    row, col = lax.axis_index("row"), lax.axis_index("col")
    me = {"x": (row % 2) * 2 + (col // 2) % 2, "y": row // 2, "z": col // 4}
    core = col % 2

    def device(at, k):
        x = at["x"]
        return (at["y"] * 2 + x // 2, at["z"] * 4 + (x % 2) * 2 + k)

    def along(dim, step, flip):
        at = dict(me)
        at[dim] = (me[dim] + step) % 4
        return at, (core + flip) % 2

    def load_in(p, h):
        return pltpu.make_async_copy(g_hbm.at[p, :, h], out.at[p, :, h], in_sem.at[p, h])

    fz_copy = pltpu.make_async_copy(fz_hbm, wbuf.at[2, pl.ds(0, 256), pl.ds(0, 256)], w_sem.at[2])
    fx_copy = pltpu.make_async_copy(fx_hbm, wbuf.at[0], w_sem.at[0])
    fy_copy = pltpu.make_async_copy(fy_hbm, wbuf.at[1], w_sem.at[1])
    load_in(0, 0).start()
    fz_copy.start()
    load_in(1, 0).start()
    load_in(2, 0).start()

    barrier = pltpu.get_barrier_semaphore()
    partners = [along(d, s, f) for d in "xyz" for s in (1, 2, 3) for f in (0, 1)]
    partners.append(along("x", 0, 1))
    for at, k in partners:
        pl.semaphore_signal(barrier, inc=1, device_id=device(at, k), device_id_type=MESH)

    def transfers(c, stage, halves):
        order = ORDER[c % 3]
        dim = order[(0, 1, 2, 2, 1, 0)[stage]]
        mine = me[dim]
        found = []
        for step in (1, 3, 2, 0):
            for flip in (0, 1) if stage in (0, 5) else (0,):
                if step == 0 and flip == 0:
                    continue
                at, k = along(dim, step, flip)
                d = at[dim]
                slot, own = d * 2 + k, mine * 2 + core
                if stage == 0:
                    pairs = [
                        (s0.at[c, h, pl.ds(slot * 128, 128)], r1.at[c, h * 8 + own]) for h in halves
                    ]
                elif stage == 1:
                    pairs = [(r1.at[c, :, pl.ds(d * 32, 32)], r2.at[c, :, mine])]
                elif stage == 2:
                    pairs = [(r2.at[c, :, :, pl.ds(d * 8, 8)], r3.at[c, :, :, mine])]
                elif stage == 3:
                    pairs = [(r3.at[c, :, :, d], b1.at[c, :, :, pl.ds(mine * 8, 8)])]
                elif stage == 4:
                    pairs = [(b1.at[c, :, d], b2.at[c, :, pl.ds(mine * 32, 32)])]
                else:
                    pairs = [
                        (b2.at[c, h * 8 + slot], b3.at[c, h, pl.ds(own * 128, 128)]) for h in halves
                    ]
                for src, dst in pairs:
                    found.append(
                        pltpu.make_async_remote_copy(
                            src, dst, send_sem.at[c, stage], recv_sem.at[c, stage],
                            device_id=device(at, k), device_id_type=MESH,
                        )
                    )
        return found

    def send(c, stage, halves=(0, 1)):
        with jax.named_scope(f"send#c={c}#s={stage}"):
            for copy in transfers(c, stage, halves):
                copy.start()
        with jax.named_scope(f"keep#c={c}#s={stage}"):
            keep(c, stage, halves)

    def keep(c, stage, halves):
        mine = me[ORDER[c % 3][(0, 1, 2, 2, 1, 0)[stage]]]
        own = mine * 2 + core
        block = pl.ds(pl.multiple_of(own * 128, 128), 128)
        part = pl.ds(pl.multiple_of(mine * 32, 32), 32)
        unit = pl.ds(pl.multiple_of(mine * 8, 8), 8)
        if stage == 0:
            for h in halves:
                r1[c, h * 8 + own] = s0[c, h, block]
        elif stage == 5:
            for h in halves:
                b3[c, h, block] = b2[c, h * 8 + own]
        else:

            @pl.loop(0, 16, unroll=4)
            def _(i):
                if stage == 1:
                    r2[c, i, mine] = r1[c, i, part]
                elif stage == 2:
                    for k in range(4):
                        r3[c, i, k, mine] = r2[c, i, k, unit]
                elif stage == 3:
                    for k in range(4):
                        b1[c, i, k, unit] = r3[c, i, k, mine]
                else:
                    b2[c, i, part] = b1[c, i, mine]

    def whole(c, stage):
        if stage == 0:
            return r1.at[c, pl.ds(0, 14)]
        if stage == 5:
            return b2.at[c, pl.ds(0, 14)]
        return (r2, r3, b1, b2)[stage - 1].at[c, pl.ds(0, 12)]

    def arrived(c, stage):
        ref = whole(c, stage)
        with jax.named_scope(f"arrive#c={c}#s={stage}"):
            pltpu.make_async_copy(ref, ref, recv_sem.at[c, stage]).wait()

    def sent(c, stage):
        ref = whole(c, stage)
        pltpu.make_async_copy(ref, ref, send_sem.at[c, stage]).wait()

    fz_copy.wait()
    fzh[...], fzl[...] = split(wbuf[2, 0:256, 0:256])

    def depth(p, j, h):
        fh, fl = fzh[j * 128 : j * 128 + 128], fzl[j * 128 : j * 128 + 128]
        for it in range(4):
            rows = [
                out[p, b, h, m * 32 : m * 32 + 32] for m in (it * 2, it * 2 + 1) for b in range(4)
            ]
            high, low = split(jnp.concatenate(rows, axis=0))

            def dot(a, b):
                return lax.dot_general(
                    a, b, (((1,), (1,)), ((), ())), preferred_element_type=F32
                )

            got = dot(fh, high) + dot(fl, high) + dot(fh, low)
            for u in range(2):
                s0[j * 3 + p, h, pl.ds(it * 2 + u, 128, stride=8)] = got[:, u * 128 : u * 128 + 128]

    for h in range(2):
        for p in range(3):
            load_in(p, h).wait()
            if h == 0:
                load_in(p, 1).start()
            with jax.named_scope(f"depth#c={p}#h={h}"):
                depth(p, 0, h)
            if h == 0 and p == 2:
                fx_copy.start()
                fy_copy.start()
                with jax.named_scope("barrier"):
                    pl.semaphore_wait(barrier, len(partners))
                for c in range(3):
                    send(c, 0, (0,))
            if h == 1:
                send(p, 0, (1,))
    for c in (3, 4, 5):
        for h in range(2):
            with jax.named_scope(f"depth#c={c}#h={h}"):
                depth(c - 3, 1, h)
        send(c, 0)

    with jax.named_scope("weights"):
        fx_copy.wait()
        fy_copy.wait()

        @pl.loop(0, 4)
        def _(i):
            at = pl.ds(pl.multiple_of(i * 128, 128), 128)
            fxh[at], fxl[at] = split(wbuf[0, at])
            turned = jnp.concatenate([wbuf[1, pl.ds(k * 128, 128), at].T for k in range(4)], axis=1)
            fyh[at], fyl[at] = split(turned)

    def units(c, r, q):
        found = []
        for e in range(4):
            at = {"x": (r % 2) * 2 + e // 2, "y": r // 2, "z": q}
            one, two, three = (at[d] for d in ORDER[c % 3])
            found.append((one * 2 + e % 2, two, three))
        return found

    def smooth(c):
        def assemble(r, q):
            for h in range(2):
                blocks = swap_blocks([r3[c, h * 8 + i, k, m] for i, k, m in units(c, r, q)])
                for b in range(4):
                    at = slice(r * 64 + b * 16 + h * 8, r * 64 + b * 16 + h * 8 + 8)
                    pbuf[at, q * 128 : q * 128 + 128] = blocks[b]

        def scatter(r, q):
            for h in range(2):
                rows = [slice(r * 64 + b * 16 + h * 8, r * 64 + b * 16 + h * 8 + 8) for b in range(4)]
                blocks = swap_blocks([pbuf[at, q * 128 : q * 128 + 128] for at in rows])
                for e, (i, k, m) in enumerate(units(c, r, q)):
                    r3[c, h * 8 + i, k, m] = blocks[e]

        for q in range(4):
            for r in range(8):
                assemble(r, q)
            cut = slice(q * 128, q * 128 + 128)
            ph[:, cut], pll[:, cut] = split(pbuf[:, cut])
        for ib in range(2):
            at = slice(ib * 256, ib * 256 + 256)
            for n in range(2):
                cut = slice(n * 256, n * 256 + 256)
                qh[at, cut], ql[at, cut] = split(dot3(fxh[at], fxl[at], ph[:, cut], pll[:, cut]))
        for ib in range(2):
            at = slice(ib * 256, ib * 256 + 256)
            for n in range(2):
                cut = slice(n * 256, n * 256 + 256)
                pbuf[at, cut] = dot3(qh[at], ql[at], fyh[:, cut], fyl[:, cut])
            for r in range(ib * 4, ib * 4 + 4):
                for q in range(4):
                    scatter(r, q)

    for stage in (1, 2):
        for c in range(6):
            arrived(c, stage - 1)
            send(c, stage)
    order = (1, 2, 0, 4, 5, 3)
    for c in order:
        arrived(c, 2)
        with jax.named_scope(f"smooth#c={c}"):
            smooth(c)
        send(c, 3)
    for stage in (4, 5):
        for c in order:
            arrived(c, stage - 1)
            send(c, stage)

    for c in range(6):
        half, p = CHUNKS[c]
        arrived(c, 5)

        with jax.named_scope(f"final#c={c}"):

            for h in range(2):
                for m in range(8):
                    turned = b3[c, h, pl.ds(m, 128, stride=8)].T
                    turned = turned * scale_ref[p : p + 1, half * 128 : half * 128 + 128]
                    for b in range(4):
                        out[p, b, h, m * 32 : m * 32 + 32, half * 128 : half * 128 + 128] = turned[
                            b * 32 : b * 32 + 32
                        ]

    with jax.named_scope("drain"):
        for c in range(6):
            for stage in range(6):
                sent(c, stage)


def shards(model_gradient, filter_x, filter_y, filter_z, depth_scale):
    params, xloc, yloc, depth = model_gradient.shape
    anywhere = pl.BlockSpec(memory_space=pl.ANY)
    result = pl.pallas_call(
        kernel,
        out_shape=pltpu.VMEM((params, 4, 2, 256, depth), F32),
        in_specs=[anywhere] * 4 + [pl.BlockSpec(memory_space=pltpu.VMEM)],
        out_specs=pl.BlockSpec(memory_space=pltpu.VMEM),
        scratch_shapes=[
            pltpu.VMEM((6, 2, 1024, 128), F32),
            pltpu.VMEM((6, 16, 128, 128), F32),
            pltpu.VMEM((6, 16, 4, 32, 128), F32),
            pltpu.VMEM((6, 16, 4, 4, 8, 128), F32),
            pltpu.VMEM((6, 16, 4, 32, 128), F32),
            pltpu.VMEM((6, 16, 128, 128), F32),
            pltpu.VMEM((6, 2, 1024, 128), F32),
            pltpu.VMEM((3, 512, 512), F32),
            pltpu.VMEM((512, 512), BF16),
            pltpu.VMEM((512, 512), BF16),
            pltpu.VMEM((512, 512), BF16),
            pltpu.VMEM((512, 512), BF16),
            pltpu.VMEM((256, 256), BF16),
            pltpu.VMEM((256, 256), BF16),
            pltpu.VMEM((512, 512), BF16),
            pltpu.VMEM((512, 512), BF16),
            pltpu.VMEM((512, 512), BF16),
            pltpu.VMEM((512, 512), BF16),
            pltpu.VMEM((512, 512), F32),
            pltpu.SemaphoreType.DMA((6, 6)),
            pltpu.SemaphoreType.DMA((6, 6)),
            pltpu.SemaphoreType.DMA((3, 2)),
            pltpu.SemaphoreType.DMA((3,)),
        ],
        compiler_params=pltpu.CompilerParams(
            collective_id=0, has_side_effects=True, vmem_limit_bytes=53 * 2**20
        ),
        name="smooth_planes",
    )(model_gradient.reshape(params, 4, 2, 256, depth), filter_x, filter_y, filter_z, depth_scale)
    return result.reshape(params, xloc, yloc, depth)


def solution(mesh):
    return jax.shard_map(
        shards,
        mesh=mesh,
        in_specs=(P(None, "row", "col", None), P(), P(), P(), P()),
        out_specs=P(None, "row", "col", None),
        check_vma=False,
    )
```

```python
import jax
import jax.numpy as jnp
from jax import lax
from jax.experimental import pallas as pl
from jax.experimental.pallas import tpu as pltpu
from jax.sharding import PartitionSpec as P

MESH = pl.DeviceIdType.MESH
F32, BF16 = jnp.float32, jnp.bfloat16
ORDER = ("xyz", "yzx", "zxy")
CHUNKS = [(half, p) for half in range(2) for p in range(3)]


def split(value):
    high = value.astype(BF16)
    return high, (value - high.astype(F32)).astype(BF16)


def swap_blocks(parts):
    lane = lax.broadcasted_iota(jnp.int32, parts[0].shape, 1)
    low64, low32 = lane < 64, lane % 64 < 32
    mid = [None] * 4
    for e in range(2):
        one, two = parts[e], parts[e + 2]
        mid[e] = jnp.where(low64, one, pltpu.roll(two, 64, 1))
        mid[e + 2] = jnp.where(low64, pltpu.roll(one, 64, 1), two)
    out = [None] * 4
    for e in (0, 2):
        one, two = mid[e], mid[e + 1]
        out[e] = jnp.where(low32, one, pltpu.roll(two, 32, 1))
        out[e + 1] = jnp.where(low32, pltpu.roll(one, 96, 1), two)
    return out


def dot3(a_high, a_low, b_high, b_low):
    def dot(a, b):
        return jnp.dot(a, b, preferred_element_type=F32)

    return dot(a_high, b_high) + dot(a_low, b_high) + dot(a_high, b_low)


def kernel(
    g_hbm, fx_hbm, fy_hbm, fz_hbm, scale_ref, out,
    s0, r1, r2, r3, b1, b2, b3,
    wbuf, fxh, fxl, fyh, fyl, fzh, fzl, ph, pll, qh, ql, pbuf,
    send_sem, recv_sem, in_sem, w_sem,
):
    row, col = lax.axis_index("row"), lax.axis_index("col")
    me = {"x": (row % 2) * 2 + (col // 2) % 2, "y": row // 2, "z": col // 4}
    core = col % 2

    def device(at, k):
        x = at["x"]
        return (at["y"] * 2 + x // 2, at["z"] * 4 + (x % 2) * 2 + k)

    def along(dim, step, flip):
        at = dict(me)
        at[dim] = (me[dim] + step) % 4
        return at, (core + flip) % 2

    def load_in(p, h):
        return pltpu.make_async_copy(g_hbm.at[p, :, h], out.at[p, :, h], in_sem.at[p, h])

    fz_copy = pltpu.make_async_copy(fz_hbm, wbuf.at[2, pl.ds(0, 256), pl.ds(0, 256)], w_sem.at[2])
    fx_copy = pltpu.make_async_copy(fx_hbm, wbuf.at[0], w_sem.at[0])
    fy_copy = pltpu.make_async_copy(fy_hbm, wbuf.at[1], w_sem.at[1])
    fz_copy.start()
    load_in(0, 0).start()

    barrier = pltpu.get_barrier_semaphore()
    partners = [along(d, s, f) for s in (2, 1, 3) for d in "xyz" for f in (0, 1)]
    partners.append(along("x", 0, 1))
    for at, k in partners:
        pl.semaphore_signal(barrier, inc=1, device_id=device(at, k), device_id_type=MESH)

    load_in(1, 0).start()

    def transfers(c, stage, halves):
        order = ORDER[c % 3]
        dim = order[(0, 1, 2, 2, 1, 0)[stage]]
        mine = me[dim]
        found = []
        for step in (1, 3, 2, 0):
            for flip in (0, 1) if stage in (0, 5) else (0,):
                if step == 0 and flip == 0:
                    continue
                at, k = along(dim, step, flip)
                d = at[dim]
                slot, own = d * 2 + k, mine * 2 + core
                if stage == 0:
                    pairs = [
                        (s0.at[c, h, pl.ds(slot * 128, 128)], r1.at[c, h * 8 + own]) for h in halves
                    ]
                elif stage == 1:
                    pairs = [(r1.at[c, :, pl.ds(d * 32, 32)], r2.at[c, :, mine])]
                elif stage == 2:
                    pairs = [(r2.at[c, :, :, pl.ds(d * 8, 8)], r3.at[c, :, :, mine])]
                elif stage == 3:
                    pairs = [(r3.at[c, :, :, d], b1.at[c, :, :, pl.ds(mine * 8, 8)])]
                elif stage == 4:
                    pairs = [(b1.at[c, :, d], b2.at[c, :, pl.ds(mine * 32, 32)])]
                else:
                    pairs = [
                        (b2.at[c, h * 8 + slot], b3.at[c, h, pl.ds(own * 128, 128)]) for h in halves
                    ]
                for i, (src, dst) in enumerate(pairs):
                    line = 6 if stage == 5 and halves[i] == 1 else stage
                    found.append(
                        pltpu.make_async_remote_copy(
                            src, dst, send_sem.at[c, stage], recv_sem.at[c, line],
                            device_id=device(at, k), device_id_type=MESH,
                        )
                    )
        return found

    def send(c, stage, halves=(0, 1)):
        with jax.named_scope(f"send#c={c}#s={stage}"):
            for copy in transfers(c, stage, halves):
                copy.start()
        with jax.named_scope(f"keep#c={c}#s={stage}"):
            keep(c, stage, halves)

    def keep(c, stage, halves):
        mine = me[ORDER[c % 3][(0, 1, 2, 2, 1, 0)[stage]]]
        own = mine * 2 + core
        block = pl.ds(pl.multiple_of(own * 128, 128), 128)
        part = pl.ds(pl.multiple_of(mine * 32, 32), 32)
        unit = pl.ds(pl.multiple_of(mine * 8, 8), 8)
        if stage == 0:
            for h in halves:
                r1[c, h * 8 + own] = s0[c, h, block]
        elif stage == 5:
            for h in halves:
                b3[c, h, block] = b2[c, h * 8 + own]
        else:

            @pl.loop(0, 16, unroll=4)
            def _(i):
                if stage == 1:
                    r2[c, i, mine] = r1[c, i, part]
                elif stage == 2:
                    for k in range(4):
                        r3[c, i, k, mine] = r2[c, i, k, unit]
                elif stage == 3:
                    for k in range(4):
                        b1[c, i, k, unit] = r3[c, i, k, mine]
                else:
                    b2[c, i, part] = b1[c, i, mine]

    def whole(c, stage):
        if stage == 0:
            return r1.at[c, pl.ds(0, 14)]
        if stage == 5:
            return b2.at[c, pl.ds(0, 14)]
        if stage == 6:
            return b2.at[c, pl.ds(0, 7)]
        return (r2, r3, b1, b2)[stage - 1].at[c, pl.ds(0, 12)]

    def arrived(c, stage):
        ref = whole(c, stage)
        with jax.named_scope(f"arrive#c={c}#s={stage}"):
            pltpu.make_async_copy(ref, ref, recv_sem.at[c, stage]).wait()

    def sent(c, stage):
        ref = whole(c, stage)
        pltpu.make_async_copy(ref, ref, send_sem.at[c, stage]).wait()

    with jax.named_scope("fz"):
        fz_copy.wait()
    fzh[...], fzl[...] = split(wbuf[2, 0:256, 0:256])

    def depth(p, j, h):
        fh, fl = fzh[j * 128 : j * 128 + 128], fzl[j * 128 : j * 128 + 128]
        rows = [out[p, b, h, m * 32 : m * 32 + 32] for m in range(8) for b in range(4)]
        high, low = split(jnp.concatenate(rows, axis=0))

        def dot(a, b):
            return lax.dot_general(a, b, (((1,), (1,)), ((), ())), preferred_element_type=F32)

        got = dot(fh, high) + dot(fl, high) + dot(fh, low)
        for m in range(8):
            s0[j * 3 + p, h, pl.ds(m, 128, stride=8)] = got[:, m * 128 : m * 128 + 128]

    for p in range(3):
        load_in(p, 0).wait()
        if p == 0:
            load_in(2, 0).start()
        else:
            load_in(p - 1, 1).start()
        with jax.named_scope(f"depth#c={p}#h=0"):
            depth(p, 0, 0)
    load_in(2, 1).start()
    with jax.named_scope("barrier"):
        pl.semaphore_wait(barrier, len(partners))
    for c in range(3):
        send(c, 0, (0,))
    fx_copy.start()
    fy_copy.start()
    for p in range(3):
        load_in(p, 1).wait()
        with jax.named_scope(f"depth#c={p}#h=1"):
            depth(p, 0, 1)
        send(p, 0, (1,))
    for c in (3, 4, 5):
        for h in range(2):
            with jax.named_scope(f"depth#c={c}#h={h}"):
                depth(c - 3, 1, h)
        send(c, 0)

    with jax.named_scope("weights"):
        fx_copy.wait()
        fy_copy.wait()

        @pl.loop(0, 4)
        def _(i):
            at = pl.ds(pl.multiple_of(i * 128, 128), 128)
            fxh[at], fxl[at] = split(wbuf[0, at])
            turned = jnp.concatenate([wbuf[1, pl.ds(k * 128, 128), at].T for k in range(4)], axis=1)
            fyh[at], fyl[at] = split(turned)

    def units(c, r, q):
        found = []
        for e in range(4):
            at = {"x": (r % 2) * 2 + e // 2, "y": r // 2, "z": q}
            one, two, three = (at[d] for d in ORDER[c % 3])
            found.append((one * 2 + e % 2, two, three))
        return found

    def smooth(c):
        def assemble(r, q):
            for h in range(2):
                blocks = swap_blocks([r3[c, h * 8 + i, k, m] for i, k, m in units(c, r, q)])
                for b in range(4):
                    at = slice(r * 64 + b * 16 + h * 8, r * 64 + b * 16 + h * 8 + 8)
                    pbuf[at, q * 128 : q * 128 + 128] = blocks[b]

        def scatter(r, q):
            for h in range(2):
                rows = [slice(r * 64 + b * 16 + h * 8, r * 64 + b * 16 + h * 8 + 8) for b in range(4)]
                blocks = swap_blocks([pbuf[at, q * 128 : q * 128 + 128] for at in rows])
                for e, (i, k, m) in enumerate(units(c, r, q)):
                    r3[c, h * 8 + i, k, m] = blocks[e]

        for q in range(4):
            for r in range(8):
                assemble(r, q)
            cut = slice(q * 128, q * 128 + 128)
            ph[:, cut], pll[:, cut] = split(pbuf[:, cut])
        for ib in range(2):
            at = slice(ib * 256, ib * 256 + 256)
            for n in range(2):
                cut = slice(n * 256, n * 256 + 256)
                qh[at, cut], ql[at, cut] = split(dot3(fxh[at], fxl[at], ph[:, cut], pll[:, cut]))
        for ib in range(2):
            at = slice(ib * 256, ib * 256 + 256)
            for n in range(2):
                cut = slice(n * 256, n * 256 + 256)
                pbuf[at, cut] = dot3(qh[at], ql[at], fyh[:, cut], fyl[:, cut])
            for r in range(ib * 4, ib * 4 + 4):
                for q in range(4):
                    scatter(r, q)

    for stage in (1, 2):
        for c in range(6):
            arrived(c, stage - 1)
            send(c, stage)
    order = (1, 2, 0, 4, 5, 3)
    for c in order:
        arrived(c, 2)
        with jax.named_scope(f"smooth#c={c}"):
            smooth(c)
        send(c, 3)
    for c in order:
        arrived(c, 3)
        send(c, 4)
    for c in order:
        arrived(c, 4)
        send(c, 5, (0,))
        send(c, 5, (1,))

    def finish(c, h):
        half, p = CHUNKS[c]
        cut = slice(half * 128, half * 128 + 128)
        for m in range(8):
            turned = b3[c, h, pl.ds(m, 128, stride=8)].T * scale_ref[p : p + 1, cut]
            for b in range(4):
                out[p, b, h, m * 32 : m * 32 + 32, cut] = turned[b * 32 : b * 32 + 32]

    def arrived_last(c, h):
        ref = whole(c, 6)
        with jax.named_scope(f"last#c={c}#h={h}"):
            pltpu.make_async_copy(ref, ref, recv_sem.at[c, 5 + h]).wait()

    for c in order[:3]:
        arrived_last(c, 0)
        finish(c, 0)
    for c in order[:3]:
        arrived_last(c, 1)
        finish(c, 1)
    with jax.named_scope("drain"):
        for c in range(6):
            for stage in range(5):
                sent(c, stage)
    for c in order[3:]:
        arrived_last(c, 0)
        finish(c, 0)
    for c in order[:3]:
        sent(c, 5)
    for c in order[3:]:
        arrived_last(c, 1)
    with jax.named_scope("final"):
        for c in order[3:]:
            finish(c, 1)
    with jax.named_scope("drain2"):
        for c in order[3:]:
            sent(c, 5)


def shards(model_gradient, filter_x, filter_y, filter_z, depth_scale):
    params, xloc, yloc, depth = model_gradient.shape
    anywhere = pl.BlockSpec(memory_space=pl.ANY)
    result = pl.pallas_call(
        kernel,
        out_shape=pltpu.VMEM((params, 4, 2, 256, depth), F32),
        in_specs=[anywhere] * 4 + [pl.BlockSpec(memory_space=pltpu.VMEM)],
        out_specs=pl.BlockSpec(memory_space=pltpu.VMEM),
        scratch_shapes=[
            pltpu.VMEM((6, 2, 1024, 128), F32),
            pltpu.VMEM((6, 16, 128, 128), F32),
            pltpu.VMEM((6, 16, 4, 32, 128), F32),
            pltpu.VMEM((6, 16, 4, 4, 8, 128), F32),
            pltpu.VMEM((6, 16, 4, 32, 128), F32),
            pltpu.VMEM((6, 16, 128, 128), F32),
            pltpu.VMEM((6, 2, 1024, 128), F32),
            pltpu.VMEM((3, 512, 512), F32),
            pltpu.VMEM((512, 512), BF16),
            pltpu.VMEM((512, 512), BF16),
            pltpu.VMEM((512, 512), BF16),
            pltpu.VMEM((512, 512), BF16),
            pltpu.VMEM((256, 256), BF16),
            pltpu.VMEM((256, 256), BF16),
            pltpu.VMEM((512, 512), BF16),
            pltpu.VMEM((512, 512), BF16),
            pltpu.VMEM((512, 512), BF16),
            pltpu.VMEM((512, 512), BF16),
            pltpu.VMEM((512, 512), F32),
            pltpu.SemaphoreType.DMA((6, 6)),
            pltpu.SemaphoreType.DMA((6, 7)),
            pltpu.SemaphoreType.DMA((3, 2)),
            pltpu.SemaphoreType.DMA((3,)),
        ],
        compiler_params=pltpu.CompilerParams(
            collective_id=0, has_side_effects=True, vmem_limit_bytes=53 * 2**20
        ),
        name="smooth_planes",
    )(model_gradient.reshape(params, 4, 2, 256, depth), filter_x, filter_y, filter_z, depth_scale)
    return result.reshape(params, xloc, yloc, depth)


def solution(mesh):
    return jax.shard_map(
        shards,
        mesh=mesh,
        in_specs=(P(None, "row", "col", None), P(), P(), P(), P()),
        out_specs=P(None, "row", "col", None),
        check_vma=False,
    )
```

```python
import jax
import jax.numpy as jnp
from jax import lax
from jax.experimental import pallas as pl
from jax.experimental.pallas import tpu as pltpu
from jax.sharding import PartitionSpec as P

MESH = pl.DeviceIdType.MESH
F32, BF16 = jnp.float32, jnp.bfloat16
ORDER = ("xyz", "yzx", "zxy")
CHUNKS = [(half, p) for half in range(2) for p in range(3)]


def split(value):
    high = value.astype(BF16)
    return high, (value - high.astype(F32)).astype(BF16)


def swap_blocks(parts):
    lane = lax.broadcasted_iota(jnp.int32, parts[0].shape, 1)
    low64, low32 = lane < 64, lane % 64 < 32
    mid = [None] * 4
    for e in range(2):
        one, two = parts[e], parts[e + 2]
        mid[e] = jnp.where(low64, one, pltpu.roll(two, 64, 1))
        mid[e + 2] = jnp.where(low64, pltpu.roll(one, 64, 1), two)
    out = [None] * 4
    for e in (0, 2):
        one, two = mid[e], mid[e + 1]
        out[e] = jnp.where(low32, one, pltpu.roll(two, 32, 1))
        out[e + 1] = jnp.where(low32, pltpu.roll(one, 96, 1), two)
    return out


def dot3(a_high, a_low, b_high, b_low):
    def dot(a, b):
        return jnp.dot(a, b, preferred_element_type=F32)

    return dot(a_high, b_high) + dot(a_low, b_high) + dot(a_high, b_low)


def kernel(
    g_hbm, fx_hbm, fy_hbm, fz_hbm, scale_ref, out,
    s0, r1, r2, r3, b1, b2, b3,
    wbuf, fxh, fxl, fyh, fyl, fzh, fzl, ph, pll, qh, ql, pbuf,
    send_sem, recv_sem, in_sem, w_sem,
):
    row, col = lax.axis_index("row"), lax.axis_index("col")
    me = {"x": (row % 2) * 2 + (col // 2) % 2, "y": row // 2, "z": col // 4}
    core = col % 2

    def device(at, k):
        x = at["x"]
        return (at["y"] * 2 + x // 2, at["z"] * 4 + (x % 2) * 2 + k)

    def along(dim, step, flip):
        at = dict(me)
        at[dim] = (me[dim] + step) % 4
        return at, (core + flip) % 2

    def load_in(p, h):
        return pltpu.make_async_copy(g_hbm.at[p, :, h], out.at[p, :, h], in_sem.at[p, h])

    fz_copy = pltpu.make_async_copy(fz_hbm, wbuf.at[2, pl.ds(0, 256), pl.ds(0, 256)], w_sem.at[2])
    fx_copy = pltpu.make_async_copy(fx_hbm, wbuf.at[0], w_sem.at[0])
    fy_copy = pltpu.make_async_copy(fy_hbm, wbuf.at[1], w_sem.at[1])
    fz_copy.start()
    load_in(0, 0).start()

    barrier = pltpu.get_barrier_semaphore()
    partners = [along(d, s, f) for s in (2, 1, 3) for d in "xyz" for f in (0, 1)]
    partners.append(along("x", 0, 1))
    for at, k in partners:
        pl.semaphore_signal(barrier, inc=1, device_id=device(at, k), device_id_type=MESH)

    load_in(1, 0).start()

    def transfers(c, stage, halves):
        order = ORDER[c % 3]
        dim = order[(0, 1, 2, 2, 1, 0)[stage]]
        mine = me[dim]
        found = []
        for step in (1, 3, 2, 0):
            for flip in (0, 1) if stage in (0, 5) else (0,):
                if step == 0 and flip == 0:
                    continue
                at, k = along(dim, step, flip)
                d = at[dim]
                slot, own = d * 2 + k, mine * 2 + core
                if stage == 0:
                    pairs = [
                        (s0.at[c, h, pl.ds(slot * 128, 128)], r1.at[c, h * 8 + own]) for h in halves
                    ]
                elif stage == 1:
                    pairs = [(r1.at[c, :, pl.ds(d * 32, 32)], r2.at[c, :, mine])]
                elif stage == 2:
                    pairs = [(r2.at[c, :, :, pl.ds(d * 8, 8)], r3.at[c, :, :, mine])]
                elif stage == 3:
                    pairs = [(r3.at[c, :, :, d], b1.at[c, :, :, pl.ds(mine * 8, 8)])]
                elif stage == 4:
                    pairs = [(b1.at[c, :, d], b2.at[c, :, pl.ds(mine * 32, 32)])]
                else:
                    pairs = [
                        (b2.at[c, h * 8 + slot], b3.at[c, h, pl.ds(own * 128, 128)]) for h in halves
                    ]
                for i, (src, dst) in enumerate(pairs):
                    line = 6 if stage == 5 and halves[i] == 1 else stage
                    found.append(
                        pltpu.make_async_remote_copy(
                            src, dst, send_sem.at[c, stage], recv_sem.at[c, line],
                            device_id=device(at, k), device_id_type=MESH,
                        )
                    )
        return found

    def send(c, stage, halves=(0, 1)):
        with jax.named_scope(f"send#c={c}#s={stage}"):
            for copy in transfers(c, stage, halves):
                copy.start()
        with jax.named_scope(f"keep#c={c}#s={stage}"):
            keep(c, stage, halves)

    def keep(c, stage, halves):
        mine = me[ORDER[c % 3][(0, 1, 2, 2, 1, 0)[stage]]]
        own = mine * 2 + core
        block = pl.ds(pl.multiple_of(own * 128, 128), 128)
        part = pl.ds(pl.multiple_of(mine * 32, 32), 32)
        unit = pl.ds(pl.multiple_of(mine * 8, 8), 8)
        if stage == 0:
            for h in halves:
                r1[c, h * 8 + own] = s0[c, h, block]
        elif stage == 5:
            for h in halves:
                b3[c, h, block] = b2[c, h * 8 + own]
        else:

            @pl.loop(0, 16, unroll=4)
            def _(i):
                if stage == 1:
                    r2[c, i, mine] = r1[c, i, part]
                elif stage == 2:
                    for k in range(4):
                        r3[c, i, k, mine] = r2[c, i, k, unit]
                elif stage == 3:
                    for k in range(4):
                        b1[c, i, k, unit] = r3[c, i, k, mine]
                else:
                    b2[c, i, part] = b1[c, i, mine]

    def whole(c, stage):
        if stage == 0:
            return r1.at[c, pl.ds(0, 14)]
        if stage == 5:
            return b2.at[c, pl.ds(0, 14)]
        if stage == 6:
            return b2.at[c, pl.ds(0, 7)]
        return (r2, r3, b1, b2)[stage - 1].at[c, pl.ds(0, 12)]

    def arrived(c, stage):
        ref = whole(c, stage)
        with jax.named_scope(f"arrive#c={c}#s={stage}"):
            pltpu.make_async_copy(ref, ref, recv_sem.at[c, stage]).wait()

    def sent(c, stage):
        ref = whole(c, stage)
        pltpu.make_async_copy(ref, ref, send_sem.at[c, stage]).wait()

    with jax.named_scope("fz"):
        fz_copy.wait()
    fzh[...], fzl[...] = split(wbuf[2, 0:256, 0:256])

    def depth(p, j, h):
        fh, fl = fzh[j * 128 : j * 128 + 128], fzl[j * 128 : j * 128 + 128]
        rows = [out[p, b, h, m * 32 : m * 32 + 32] for m in range(8) for b in range(4)]
        high, low = split(jnp.concatenate(rows, axis=0))

        def dot(a, b):
            return lax.dot_general(a, b, (((1,), (1,)), ((), ())), preferred_element_type=F32)

        got = dot(fh, high) + dot(fl, high) + dot(fh, low)
        for m in range(8):
            s0[j * 3 + p, h, pl.ds(m, 128, stride=8)] = got[:, m * 128 : m * 128 + 128]

    for p in range(3):
        load_in(p, 0).wait()
        if p == 0:
            load_in(2, 0).start()
        else:
            load_in(p - 1, 1).start()
        with jax.named_scope(f"depth#c={p}#h=0"):
            depth(p, 0, 0)
    load_in(2, 1).start()
    with jax.named_scope("barrier"):
        pl.semaphore_wait(barrier, len(partners))
    for c in range(3):
        send(c, 0, (0,))
    fx_copy.start()
    fy_copy.start()
    for p in range(3):
        load_in(p, 1).wait()
        with jax.named_scope(f"depth#c={p}#h=1"):
            depth(p, 0, 1)
        send(p, 0, (1,))
    for c in (3, 4, 5):
        for h in range(2):
            with jax.named_scope(f"depth#c={c}#h={h}"):
                depth(c - 3, 1, h)
        send(c, 0)

    with jax.named_scope("weights"):
        fx_copy.wait()
        fy_copy.wait()

        @pl.loop(0, 4)
        def _(i):
            at = pl.ds(pl.multiple_of(i * 128, 128), 128)
            fxh[at], fxl[at] = split(wbuf[0, at])
            turned = jnp.concatenate([wbuf[1, pl.ds(k * 128, 128), at].T for k in range(4)], axis=1)
            fyh[at], fyl[at] = split(turned)

    def units(c, r, q):
        found = []
        for e in range(4):
            at = {"x": (r % 2) * 2 + e // 2, "y": r // 2, "z": q}
            one, two, three = (at[d] for d in ORDER[c % 3])
            found.append((one * 2 + e % 2, two, three))
        return found

    def smooth(c):
        def assemble(r, q):
            for h in range(2):
                blocks = swap_blocks([r3[c, h * 8 + i, k, m] for i, k, m in units(c, r, q)])
                for b in range(4):
                    at = slice(r * 64 + b * 16 + h * 8, r * 64 + b * 16 + h * 8 + 8)
                    pbuf[at, q * 128 : q * 128 + 128] = blocks[b]

        def scatter(r, q):
            for h in range(2):
                rows = [slice(r * 64 + b * 16 + h * 8, r * 64 + b * 16 + h * 8 + 8) for b in range(4)]
                blocks = swap_blocks([pbuf[at, q * 128 : q * 128 + 128] for at in rows])
                for e, (i, k, m) in enumerate(units(c, r, q)):
                    r3[c, h * 8 + i, k, m] = blocks[e]

        for q in range(4):
            for r in range(8):
                assemble(r, q)
            cut = slice(q * 128, q * 128 + 128)
            ph[:, cut], pll[:, cut] = split(pbuf[:, cut])
        for ib in range(2):
            at = slice(ib * 256, ib * 256 + 256)
            for n in range(2):
                cut = slice(n * 256, n * 256 + 256)
                qh[at, cut], ql[at, cut] = split(dot3(fxh[at], fxl[at], ph[:, cut], pll[:, cut]))
        for ib in range(2):
            at = slice(ib * 256, ib * 256 + 256)
            for n in range(2):
                cut = slice(n * 256, n * 256 + 256)
                pbuf[at, cut] = dot3(qh[at], ql[at], fyh[:, cut], fyl[:, cut])
            for r in range(ib * 4, ib * 4 + 4):
                for q in range(4):
                    scatter(r, q)

    for stage in (1, 2):
        for c in range(6):
            arrived(c, stage - 1)
            send(c, stage)
    order = (1, 2, 0, 4, 5, 3)
    for c in order:
        arrived(c, 2)
        with jax.named_scope(f"smooth#c={c}"):
            smooth(c)
        send(c, 3)
    for c in order:
        arrived(c, 3)
        send(c, 4)
    for c in order:
        arrived(c, 4)
        send(c, 5, (0,))
        send(c, 5, (1,))

    def finish(c, h):
        half, p = CHUNKS[c]
        cut = slice(half * 128, half * 128 + 128)
        for m in range(8):
            turned = b3[c, h, pl.ds(m, 128, stride=8)].T * scale_ref[p : p + 1, cut]
            for b in range(4):
                out[p, b, h, m * 32 : m * 32 + 32, cut] = turned[b * 32 : b * 32 + 32]

    def arrived_last(c, h):
        ref = whole(c, 6)
        with jax.named_scope(f"last#c={c}#h={h}"):
            pltpu.make_async_copy(ref, ref, recv_sem.at[c, 5 + h]).wait()

    for c in order[:3]:
        arrived_last(c, 0)
        finish(c, 0)
    for c in order[:3]:
        arrived_last(c, 1)
        finish(c, 1)
    with jax.named_scope("drain"):
        for c in range(6):
            for stage in range(5):
                sent(c, stage)
    for c in order[3:]:
        arrived_last(c, 0)
        finish(c, 0)
    for c in order[:3]:
        sent(c, 5)
    for c in order[3:]:
        arrived_last(c, 1)
    with jax.named_scope("final"):
        for c in order[3:]:
            finish(c, 1)
    with jax.named_scope("drain2"):
        for c in order[3:]:
            sent(c, 5)


def write_out(held, out_hbm, sem):
    copies = [
        pltpu.make_async_copy(held.at[p, b], out_hbm.at[p, b], sem.at[p, b])
        for p in range(held.shape[0])
        for b in range(4)
    ]
    for copy in copies:
        copy.start()
    for copy in copies:
        copy.wait()


def shards(model_gradient, filter_x, filter_y, filter_z, depth_scale):
    params, xloc, yloc, depth = model_gradient.shape
    anywhere = pl.BlockSpec(memory_space=pl.ANY)
    result = pl.pallas_call(
        kernel,
        out_shape=pltpu.VMEM((params, 4, 2, 256, depth), F32),
        in_specs=[anywhere] * 4 + [pl.BlockSpec(memory_space=pltpu.VMEM)],
        out_specs=pl.BlockSpec(memory_space=pltpu.VMEM),
        scratch_shapes=[
            pltpu.VMEM((6, 2, 1024, 128), F32),
            pltpu.VMEM((6, 16, 128, 128), F32),
            pltpu.VMEM((6, 16, 4, 32, 128), F32),
            pltpu.VMEM((6, 16, 4, 4, 8, 128), F32),
            pltpu.VMEM((6, 16, 4, 32, 128), F32),
            pltpu.VMEM((6, 16, 128, 128), F32),
            pltpu.VMEM((6, 2, 1024, 128), F32),
            pltpu.VMEM((3, 512, 512), F32),
            pltpu.VMEM((512, 512), BF16),
            pltpu.VMEM((512, 512), BF16),
            pltpu.VMEM((512, 512), BF16),
            pltpu.VMEM((512, 512), BF16),
            pltpu.VMEM((256, 256), BF16),
            pltpu.VMEM((256, 256), BF16),
            pltpu.VMEM((512, 512), BF16),
            pltpu.VMEM((512, 512), BF16),
            pltpu.VMEM((512, 512), BF16),
            pltpu.VMEM((512, 512), BF16),
            pltpu.VMEM((512, 512), F32),
            pltpu.SemaphoreType.DMA((6, 6)),
            pltpu.SemaphoreType.DMA((6, 7)),
            pltpu.SemaphoreType.DMA((3, 2)),
            pltpu.SemaphoreType.DMA((3,)),
        ],
        compiler_params=pltpu.CompilerParams(
            collective_id=0, has_side_effects=True, vmem_limit_bytes=53 * 2**20
        ),
        name="smooth_planes",
    )(model_gradient.reshape(params, 4, 2, 256, depth), filter_x, filter_y, filter_z, depth_scale)
    result = pltpu.with_memory_space_constraint(result, pltpu.VMEM)
    result = pl.pallas_call(
        write_out,
        out_shape=jax.ShapeDtypeStruct((params, 4, 2, 256, depth), F32),
        in_specs=[pl.BlockSpec(memory_space=pltpu.VMEM)],
        out_specs=anywhere,
        scratch_shapes=[pltpu.SemaphoreType.DMA((params, 4))],
        compiler_params=pltpu.CompilerParams(vmem_limit_bytes=16 * 2**20),
        name="write_out",
    )(result)
    return result.reshape(params, xloc, yloc, depth)


def solution(mesh):
    return jax.shard_map(
        shards,
        mesh=mesh,
        in_specs=(P(None, "row", "col", None), P(), P(), P(), P()),
        out_specs=P(None, "row", "col", None),
        check_vma=False,
    )
```
